32 devices in a mesh: seq: 16 (over z, y, core), head: 2 (over x).
Axes of the slice: x: 2, y: 2, z: 4, core: 2. Of those that a mesh axis runs over, the one named last changes fastest.
Arguments:
- query: bfloat16 [4096, 2048], P('seq', 'head'), may hold values from -4.5 to 4.5
- key_value: bfloat16 [4096, 512], P('seq'), may hold values from -4.5 to 4.5
- out_grad: bfloat16 [4096, 2048], P('seq', 'head'), may hold values from -48 to 48
- inputs_normed: bfloat16 [4096, 4096], P('seq'), may hold values from -8 to 8
- kv_weight: bfloat16 [2, 4096, 256], P(None, 'head'), may hold values from -0.09375 to 0.09375
- segment_ids: int32 [4096], replicated, may hold values from 0 to 2, never falling along the last dimension, each value on 1 to 2048 neighbouring positions
Outputs:
- query_grad: bfloat16 [4096, 2048], P('seq', 'head')
- input_grad: bfloat16 [4096, 4096], P('seq', 'head')
- weight_grad: float32 [2, 4096, 256], P('head', 'seq')
The draws below stay inside these ranges and needn't reach their ends.
All inputs are finite; a program needn't handle non-finite values.
Results may differ from the reference program's by a relative error of at most 0.015.
Values may be sent and summed in bfloat16 or wider, within the bound.
A program may use at most 64 MiB of HBM per device.

```python
import math
import jax
import jax.numpy as jnp
import numpy as np
from jax import lax

D = 4096
H = 8
HD = 256
WIN = 2048
TOK_DEV = 256
TOKENS = 4096


def draw_query(key, part):
    base_draw = jnp.clip(jax.random.normal(jax.random.fold_in(key, 13), (TOKENS, H * HD)), -4.5, 4.5)
    return base_draw.astype(jnp.bfloat16)


def draw_key_value(key, part):
    key_part = jnp.clip(jax.random.normal(jax.random.fold_in(key, 11), (TOKENS, HD)), -4.5, 4.5)
    value_part = jnp.clip(jax.random.normal(jax.random.fold_in(key, 12), (TOKENS, HD)), -4.5, 4.5)
    return jnp.concatenate([key_part, value_part], axis=1).astype(jnp.bfloat16)


def with_spikes(values, rng, source, target, blocks, factor):
    owner, partner = [(jnp.arange(values.shape[dim]) // (values.shape[dim] // blocks)).reshape([-1 if axis == dim else 1 for axis in range(values.ndim)]) for dim in (source, target)]
    chosen = jax.random.permutation(rng, blocks)[partner]
    strong = (owner == chosen) | (owner == (partner + blocks // 2) % blocks)
    return jnp.where(strong, factor * values, values)


def level_of(rng, shape, cuts, smallest, largest):
    factor_of = 1.0
    for position, parts in cuts:
        steps = jax.random.uniform(jax.random.fold_in(jax.random.fold_in(rng, 6), position), (parts,), jnp.float32, smallest / len(cuts), largest / len(cuts))
        factor_of = factor_of * jnp.repeat(jnp.exp(steps), shape[position] // parts).reshape((-1,) + (1,) * (len(shape) - 1 - position))
    return factor_of


def split_up(number_of, total, limit, skew):
    loads = [(1 << 20) // math.isqrt(rank ** skew) + 1 for rank in range(2, number_of + 1)]
    spare, counts = total - limit - (number_of - 1), [1] * (number_of - 1)
    while spare > 0:
        free = [i for i in range(number_of - 1) if counts[i] < limit]
        whole, left = sum([loads[i] for i in free]), spare
        for i in free:
            addition = min(limit - counts[i], max(1, left * loads[i] // whole), spare)
            counts[i] = counts[i] + addition
            spare = spare - addition
    return np.array([limit] + counts)


def ragged_sizes(own_key, count, total, reach, lean):
    if count == 2:
        one = jax.random.randint(own_key, (), max(1, total - reach), min(reach, total - 1) + 1)
        return jnp.stack([one, total - one])
    sizes = jnp.asarray(split_up(count, total, reach, lean), jnp.int32)
    twos = (count - 1) // 2
    giver, taker = sizes[1:1 + 2 * twos:2], sizes[2:2 + 2 * twos:2]
    room = jnp.minimum(giver - 1, reach - taker)
    passed = jax.random.randint(jax.random.fold_in(own_key, 1), (twos,), 0, 1 << 20) % (room + 1)
    sizes = sizes.at[1:1 + 2 * twos:2].set(giver - passed).at[2:2 + 2 * twos:2].set(taker + passed)
    return sizes[jax.random.permutation(jax.random.fold_in(own_key, 2), count)]


def normal_values(own_key, extent, scale, reach, pieces=(), kind=jnp.bfloat16):
    level = level_of(own_key, extent, pieces, -0.22, 0.18) if pieces else 1.0
    entries = jax.random.normal(own_key, extent, jnp.float32) * scale * level
    return jnp.minimum(jnp.maximum(entries, -reach), reach).astype(kind)


def noise_with(key, dims, width, most, cuts, heavy, kind=jnp.bfloat16):
    drawn = width * jax.random.normal(key, dims, jnp.float32)
    if cuts:
        drawn = drawn * level_of(key, dims, cuts, -0.22, 0.18)
    return jnp.clip(with_spikes(drawn, jax.random.fold_in(key, 3), *heavy), -most, most).astype(kind)


def setup_inputs(seed: int = 0) -> dict:
    key_of = jax.random.split(jax.random.key(seed), 7)
    return {
        "query": draw_query(jax.random.fold_in(key_of[6], 71), 0),
        "key_value": draw_key_value(jax.random.fold_in(key_of[6], 71), 0),
        "out_grad": normal_values(key_of[2], (TOKENS, H * HD), 8.0, 48.0, ((0, 16), (1, 2))),
        "inputs_normed": noise_with(key_of[3], (TOKENS, D), 1.0, 8.0, ((0, 16),), (0, 1, 16, 2.0)),
        "kv_weight": normal_values(key_of[4], (2, D, HD), D ** -0.5, 0.09375, ((1, 2),)),
        "segment_ids": jnp.searchsorted(jnp.cumsum(ragged_sizes(key_of[5], max(3, TOKENS // (2 * WIN)), TOKENS, min(4 * WIN, TOKENS - WIN), 1)), jnp.arange(TOKENS), side="right").astype(jnp.int32),
    }


def attention_block(query_rows, out_rows, window, allowed, head_count):
    head_dim = window.shape[1] // 2
    tok_rows = query_rows.shape[0]
    inv_root = 1.0 / math.sqrt(head_dim)
    key_rows = window[:, :head_dim]
    value_rows = window[:, head_dim:]
    flat_q = query_rows.reshape(tok_rows * head_count, head_dim)
    flat_do = out_rows.reshape(tok_rows * head_count, head_dim)
    scores = jnp.dot(flat_q, key_rows.T, preferred_element_type=jnp.float32) * inv_root
    scores = scores.reshape(tok_rows, head_count, -1)
    masked = jnp.where(allowed[:, None, :], scores, -jnp.inf)
    row_max = lax.optimization_barrier(jnp.max(masked, axis=-1, keepdims=True))
    shifted = jnp.exp(masked - row_max)
    probabilities = (shifted / lax.optimization_barrier(jnp.sum(shifted, axis=-1, keepdims=True))).reshape(tok_rows * head_count, -1)
    prob_bf16 = probabilities.astype(jnp.bfloat16)
    attended = jnp.dot(prob_bf16, value_rows, preferred_element_type=jnp.float32)
    row_delta = lax.optimization_barrier(jnp.sum(flat_do.astype(jnp.float32) * attended, axis=-1, keepdims=True))
    prob_grad = jnp.dot(flat_do, value_rows.T, preferred_element_type=jnp.float32)
    dscore_b = (probabilities * (prob_grad - row_delta)).astype(jnp.bfloat16)
    query_grad = (jnp.dot(dscore_b, key_rows, preferred_element_type=jnp.float32) * inv_root).astype(jnp.bfloat16)
    query_grad = query_grad.reshape(tok_rows, head_count * head_dim)
    key_grad = jnp.dot(dscore_b.T, flat_q, preferred_element_type=jnp.float32) * inv_root
    value_grad = jnp.dot(prob_bf16.T, flat_do, preferred_element_type=jnp.float32)
    return (query_grad, jnp.concatenate([key_grad, value_grad], axis=1))

def reference(query, key_value, out_grad, inputs_normed, kv_weight, segment_ids):
    tok_rows = TOK_DEV
    span = WIN + tok_rows
    block_count = TOKENS // tok_rows
    padded_kv = jnp.concatenate([jnp.zeros((WIN, 2 * HD), key_value.dtype), key_value], axis=0)
    padded_seg = jnp.concatenate([jnp.full((WIN,), -1, jnp.int32), segment_ids.astype(jnp.int32)], axis=0)

    def one_block(accumulated, block_index):
        begin_row = (block_index * tok_rows).astype(jnp.int32)
        window = lax.dynamic_slice_in_dim(padded_kv, begin_row, span, 0)
        key_seg = lax.dynamic_slice_in_dim(padded_seg, begin_row, span, 0)
        query_seg = lax.dynamic_slice_in_dim(segment_ids.astype(jnp.int32), begin_row, tok_rows, 0)
        query_pos = begin_row + jnp.arange(tok_rows, dtype=jnp.int32)
        key_pos = begin_row - WIN + jnp.arange(span, dtype=jnp.int32)
        distance = query_pos[:, None] - key_pos[None, :]
        allowed = (distance >= 0) & (distance < WIN) & (query_seg[:, None] == key_seg[None, :])
        query_rows = lax.dynamic_slice_in_dim(query, begin_row, tok_rows, 0)
        out_rows = lax.dynamic_slice_in_dim(out_grad, begin_row, tok_rows, 0)
        query_grad, window_grad = attention_block(query_rows, out_rows, window, allowed, H)
        old_part = lax.dynamic_slice_in_dim(accumulated, begin_row, span, 0)
        accumulated = lax.dynamic_update_slice_in_dim(accumulated, old_part + window_grad, begin_row, 0)
        return (accumulated, query_grad)
    start_sum = jnp.zeros((WIN + TOKENS, 2 * HD), jnp.float32)
    accumulated, query_blocks = lax.scan(one_block, start_sum, jnp.arange(block_count, dtype=jnp.int32))
    query_grad = query_blocks.reshape(TOKENS, H * HD)
    kv_grad = accumulated[WIN:].astype(jnp.bfloat16)
    stacked_weight = jnp.concatenate([kv_weight[0], kv_weight[1]], axis=1)
    input_grad = jnp.dot(kv_grad, stacked_weight.T, preferred_element_type=jnp.float32).astype(jnp.bfloat16)
    norm_factor = 1.0 / math.sqrt(TOKENS)
    key_weight = jnp.dot(inputs_normed.T, kv_grad[:, :HD], preferred_element_type=jnp.float32) * norm_factor
    value_weight = jnp.dot(inputs_normed.T, kv_grad[:, HD:], preferred_element_type=jnp.float32) * norm_factor
    weight_grad = jnp.stack([key_weight, value_weight], axis=0)
    return (query_grad, input_grad, weight_grad)
```

```python
import functools
import math

import jax
import jax.numpy as jnp
from jax import lax
from jax.experimental import pallas as pl
from jax.experimental.pallas import tpu as pltpu
from jax.sharding import PartitionSpec as P

WIN = 2048
MESH = pl.DeviceIdType.MESH
F32 = jnp.float32
BF16 = jnp.bfloat16
NT = (((1,), (1,)), ((), ()))
TN = (((0,), (0,)), ((), ()))


def dot(a, b, dims=(((1,), (0,)), ((), ()))):
    return lax.dot_general(a, b, dims, preferred_element_type=F32)


def kernel(planes, rows_out, heads, norm, q_ref, kv_ref, do_ref, lo_ref, x_hbm, w_hbm,
           dq_ref, ig_ref, wg_ref,
           win, qf, dof, sc, dp, pb, ds, acc, gs, rc, ys, yr, zs, zr, xs, xr, mh, oh,
           xv, wv, xt, wb, wa, cr, yw, ywr, zw, zwr,
           loc_sem, own_sem, zsend, zrecv, ysend, yrecv, csend, crecv,
           gsend, grecv, bysend, byrecv, bzsend, bzrecv, bxsend, bxrecv,
           wcsend, wcrecv, wysend, wyrecv, wzsend, wzrecv):
    tok = q_ref.shape[0]
    hd = kv_ref.shape[1] // 2
    nblk = WIN // tok + 1
    s_idx = lax.axis_index("seq")
    h_idx = lax.axis_index("head")
    k = s_idx % 2
    y = (s_idx // 2) % 2
    p = s_idx // 4
    core_dev = ((p * 2 + y) * 2 + 1 - k, h_idx)
    y_dev = ((p * 2 + 1 - y) * 2 + k, h_idx)
    x_dev = (s_idx, 1 - h_idx)

    def plane_dev(step):
        return ((((p + step) % planes) * 2 + y) * 2 + k, h_idx)

    next_dev = plane_dev(1)
    prev_dev = plane_dev(planes - 1)

    load_x = pltpu.make_async_copy(x_hbm, xv, loc_sem.at[0])
    load_w = pltpu.make_async_copy(w_hbm, wv, loc_sem.at[1])
    load_x.start()
    load_w.start()

    barrier = pltpu.get_barrier_semaphore()
    for dev in [core_dev, y_dev, x_dev] + [plane_dev(t) for t in range(1, planes)]:
        pl.semaphore_signal(barrier, inc=1, device_id=dev, device_id_type=MESH)
    pl.semaphore_wait(barrier, planes + 2)

    def remote(src, dst, ssem, rsem, dev):
        return pltpu.make_async_remote_copy(
            src_ref=src, dst_ref=dst, send_sem=ssem, recv_sem=rsem,
            device_id=dev, device_id_type=MESH)

    def slot(half, j, core):
        return win.at[half, pl.ds(((4 - j) * 2 + core) * tok, tok)]

    def kv_half(half):
        return kv_ref.at[:, pl.ds(half * hd, hd)]

    def z_own(half):
        return remote(kv_half(half), slot(half, 2, k), zsend.at[0, half], zrecv.at[0, half], next_dev)

    def z_relay(half):
        return remote(slot(half, 2, k), slot(half, 4, k), zsend.at[1, half], zrecv.at[1, half], next_dev)

    def y_first(half, src):
        return remote(src, slot(half, 1, k), ysend.at[0, half], yrecv.at[0, half], y_dev)

    def y_second(half, j):
        return remote(slot(half, j, k), slot(half, 3, k), ysend.at[1, half], yrecv.at[1, half], y_dev)

    def to_core(half, j, src):
        return remote(src, slot(half, j, k), csend.at[j, half], crecv.at[j, half], core_dev)

    def own_fill(half):
        return pltpu.make_async_copy(kv_half(half), slot(half, 0, k), own_sem.at[half])

    def sends_core(j):
        return k == 0 if j == 0 else (k == 1 if j == 4 else None)

    def start_core(half, j, src):
        cond = sends_core(j)
        if cond is None:
            to_core(half, j, src).start()
        else:
            pl.when(cond)(lambda: to_core(half, j, src).start())

    for half in range(2):
        z_own(half).start()
        pl.when(y == 0)(lambda half=half: y_first(half, kv_half(half)).start())
        own_fill(half).start()
        start_core(half, 0, kv_half(half))

    for h in range(heads):
        qf[h * tok:(h + 1) * tok, :] = q_ref[:, h * hd:(h + 1) * hd]
        dof[h * tok:(h + 1) * tok, :] = do_ref[:, h * hd:(h + 1) * hd]

    for half in range(2):
        z_own(half).wait_recv()
        z_relay(half).start()

        @pl.when(y == 0)
        def _(half=half):
            y_second(half, 2).start()

        @pl.when(y == 1)
        def _(half=half):
            y_first(half, slot(half, 2, k)).start()

        start_core(half, 2, slot(half, 2, k))

    load_x.wait()
    per = max(1, 256 // rows_out)
    wide = per * rows_out
    for i in range(xv.shape[1] // wide):
        piece = xv[:, i * wide:(i + 1) * wide].T
        for u in range(per):
            dest = i * per + u
            place = ((dest % 2) * 2 + (dest // 2) % 2) * planes + dest // 4
            xt[place * rows_out:(place + 1) * rows_out, :] = piece[u * rows_out:(u + 1) * rows_out]

    for half in range(2):
        y_first(half, kv_half(half)).wait_recv()
        start_core(half, 1, slot(half, 1, k))
    for half in range(2):
        z_relay(half).wait_recv()
        pl.when(y == 1)(lambda half=half: y_second(half, 4).start())
        start_core(half, 4, slot(half, 4, k))
    for half in range(2):
        y_second(half, 2).wait_recv()
        start_core(half, 3, slot(half, 3, k))
    for half in range(2):
        own_fill(half).wait()
        for j in range(1, 4):
            to_core(half, j, slot(half, j, k)).wait_recv()
        pl.when(k == 1)(lambda half=half: to_core(half, 0, slot(half, 0, k)).wait_recv())
        pl.when(k == 0)(lambda half=half: to_core(half, 4, slot(half, 4, k)).wait_recv())

    lo = lo_ref[...]
    hi = lax.broadcasted_iota(jnp.int32, (1, tok), 1) + WIN
    inv_root = 1.0 / math.sqrt(hd)

    def block_rows(d):
        return pl.ds(pl.multiple_of((k + d) * tok, tok), tok)

    def own_rows(d):
        return pl.ds(pl.multiple_of(d * tok, tok), tok)

    def pass_scores(d, tops):
        keys = win[0, block_rows(d), :]
        r = lax.broadcasted_iota(jnp.int32, (tok, tok), 0) + d * tok
        ok = (r >= lo) & (r <= hi)
        out = []
        for h in range(heads):
            s = dot(keys, qf[h * tok:(h + 1) * tok, :], NT) * inv_root
            s = jnp.where(ok, s, -jnp.inf)
            sc[own_rows(d), h * tok:(h + 1) * tok] = s
            out.append(jnp.maximum(tops[h], jnp.max(s, axis=0, keepdims=True)))
        return tuple(out)

    tops = lax.fori_loop(
        0, nblk, pass_scores, tuple(jnp.full((1, tok), -jnp.inf, F32) for _ in range(heads)))

    def pass_exp(d, sums):
        vals = win[1, block_rows(d), :]
        out = []
        for h in range(heads):
            cols = slice(h * tok, (h + 1) * tok)
            e = jnp.exp(sc[own_rows(d), cols] - tops[h])
            g = dot(vals, dof[cols, :], NT)
            sc[own_rows(d), cols] = e
            dp[own_rows(d), cols] = g
            out.append((sums[h][0] + jnp.sum(e, axis=0, keepdims=True),
                        sums[h][1] + jnp.sum(e * g, axis=0, keepdims=True)))
        return tuple(out)

    zero = jnp.zeros((1, tok), F32)
    sums = lax.fori_loop(0, nblk, pass_exp, tuple((zero, zero) for _ in range(heads)))
    invs = [1.0 / total for total, _ in sums]
    deltas = [part * inv for (_, part), inv in zip(sums, invs)]

    def pass_grad(d):
        for h in range(heads):
            cols = slice(h * tok, (h + 1) * tok)
            prob = sc[own_rows(d), cols] * invs[h]
            pb[own_rows(d), cols] = prob.astype(BF16)
            ds[own_rows(d), cols] = (prob * (dp[own_rows(d), cols] - deltas[h])).astype(BF16)

    def grad_of(d, half):
        if half == 0:
            return dot(ds[own_rows(d), :], qf[...]) * inv_root
        return dot(pb[own_rows(d), :], dof[...])

    def g_copy(m, half):
        return remote(gs.at[m, half], rc.at[m, half], gsend.at[m, half], grecv.at[m, half], core_dev)

    def grad_pair(m):
        pass_grad(2 * m + 1)
        for half in range(2):
            gs[m, half] = grad_of(2 * m + 1, half).astype(BF16)
            g_copy(m, half).start()
        pass_grad(2 * m)
        for half in range(2):
            acc[4 - m, half] = grad_of(2 * m, half)

    def add_core(m):
        for half in range(2):
            g_copy(m, half).wait_recv()
            acc[3 - m + k, half] = acc[3 - m + k, half] + rc[m, half].astype(F32)

    def y_copy(i, half):
        return remote(ys.at[i, half], yr.at[i, half], bysend.at[i, half], byrecv.at[i, half], y_dev)

    def z_copy(i, half):
        return remote(zs.at[i, half], zr.at[i, half], bzsend.at[i, half], bzrecv.at[i, half], prev_dev)

    grad_pair(0)
    grad_pair(1)
    grad_pair(2)
    add_core(0)
    add_core(1)
    for half in range(2):
        ys[1, half] = acc[3, half].astype(BF16)
        y_copy(1, half).start()
    grad_pair(3)
    pass_grad(8)
    for half in range(2):
        acc[0, half] = grad_of(8, half)
    add_core(2)
    add_core(3)
    for half in range(2):
        ys[0, half] = acc[1, half].astype(BF16)
        y_copy(0, half).start()
    for half in range(2):
        y_copy(1, half).wait_recv()
        acc[2 + 2 * y, half] = acc[2 + 2 * y, half] + yr[1, half].astype(F32)
        zs[1, half] = acc[4, half].astype(BF16)
        z_copy(1, half).start()
    for h in range(heads):
        cols = slice(h * tok, (h + 1) * tok)
        keys = win[0, pl.ds(pl.multiple_of(k * tok, tok), nblk * tok), :]
        dq_ref[:, h * hd:(h + 1) * hd] = (dot(ds[:, cols], keys, TN) * inv_root).astype(BF16)
    for half in range(2):
        y_copy(0, half).wait_recv()
        acc[2 * y, half] = acc[2 * y, half] + yr[0, half].astype(F32)
        z_copy(1, half).wait_recv()
        zs[0, half] = (acc[2, half] + zr[1, half].astype(F32)).astype(BF16)
        z_copy(0, half).start()
    for half in range(2):
        z_copy(0, half).wait_recv()
        acc[0, half] = acc[0, half] + zr[0, half].astype(F32)

    x_half = remote(xs, xr, bxsend.at[0], bxrecv.at[0], x_dev)
    x_back = remote(mh, oh, bxsend.at[1], bxrecv.at[1], x_dev)
    xs[...] = acc[0, 1 - h_idx].astype(BF16)
    x_half.start()
    x_half.wait_recv()
    mh[...] = (acc[0, h_idx] + xr[...].astype(F32)).astype(BF16)
    x_back.start()

    group = planes * rows_out
    half_rows = 2 * group

    def w_core(i):
        return remote(wb.at[i], cr.at[i], wcsend.at[i], wcrecv.at[i], core_dev)

    def xt_rows(core, yy):
        return xt[pl.ds(pl.multiple_of((core * 2 + yy) * group, group), group), :]

    def w_y(t):
        return remote(yw.at[t], ywr.at[t], wysend.at[t], wyrecv.at[t], y_dev)

    def w_z(t):
        return remote(zw.at[t], zwr.at[t], wzsend.at[t], wzrecv.at[t], plane_dev(t))

    for i in range(2):
        yy = 1 - y if i == 0 else y
        wb[i] = dot(xt_rows(1 - k, yy), mh[...]).astype(BF16)
        w_core(i).start()
    for i in range(2):
        yy = 1 - y if i == 0 else y
        wa[i] = dot(xt_rows(k, yy), mh[...])

    order = list(range(1, planes)) + [0]

    def plane_rows(t):
        return pl.ds(pl.multiple_of(((p + t) % planes) * rows_out, rows_out), rows_out)

    w_core(0).wait_recv()
    for t in order:
        yw[t] = (wa[0, plane_rows(t), :] + cr[0, plane_rows(t), :].astype(F32)).astype(BF16)
        w_y(t).start()
    w_core(1).wait_recv()
    wa[1] = wa[1] + cr[1].astype(F32)

    load_w.wait()
    x_back.wait_recv()
    first = jnp.where(h_idx == 0, mh[...].astype(F32), oh[...].astype(F32)).astype(BF16)
    second = jnp.where(h_idx == 0, oh[...].astype(F32), mh[...].astype(F32)).astype(BF16)
    width = wv.shape[1]
    step = 512
    for i in range(width // step):
        cols = slice(i * step, (i + 1) * step)
        ig_ref[:, cols] = (dot(first, wv[0, cols, :], NT) + dot(second, wv[1, cols, :], NT)).astype(BF16)

    for t in order[:-1]:
        w_y(t).wait_recv()
        zw[t] = (wa[1, plane_rows(t), :] + ywr[t].astype(F32)).astype(BF16)
        w_z(t).start()
    w_y(0).wait_recv()
    total = wa[1, plane_rows(0), :] + ywr[0].astype(F32)
    for t in order[:-1]:
        w_z(t).wait_recv()
        total = total + zwr[t].astype(F32)
    wg_ref[...] = total * norm

    for half in range(2):
        z_own(half).wait_send()
        z_relay(half).wait_send()
        y_first(half, kv_half(half)).wait_send()
        y_second(half, 2).wait_send()
        for j in range(1, 4):
            to_core(half, j, slot(half, j, k)).wait_send()
        pl.when(k == 0)(lambda half=half: to_core(half, 0, slot(half, 0, k)).wait_send())
        pl.when(k == 1)(lambda half=half: to_core(half, 4, slot(half, 4, k)).wait_send())
        for m in range(4):
            g_copy(m, half).wait_send()
        for i in range(2):
            y_copy(i, half).wait_send()
            z_copy(i, half).wait_send()
    x_half.wait_send()
    x_back.wait_send()
    for i in range(2):
        w_core(i).wait_send()
    for t in order:
        w_y(t).wait_send()
    for t in order[:-1]:
        w_z(t).wait_send()


def local(query, key_value, out_grad, inputs_normed, kv_weight, segment_ids):
    tok = query.shape[0]
    hd = key_value.shape[1] // 2
    heads = query.shape[1] // hd
    seqs = lax.axis_size("seq")
    planes = seqs // 4
    width = inputs_normed.shape[1]
    rows_out = width // seqs
    span = WIN + tok
    nblk = span // tok
    group = planes * rows_out
    begin = lax.axis_index("seq") * tok
    padded = jnp.concatenate([jnp.full((WIN,), -1, jnp.int32), segment_ids])
    key_seg = lax.dynamic_slice_in_dim(padded, begin, span, 0)
    earlier = jnp.sum((key_seg[:, None] < key_seg[None, WIN:]).astype(jnp.int32), axis=0)
    lo = jnp.maximum(earlier, jnp.arange(tok, dtype=jnp.int32) + 1)[None]
    norm = 1.0 / math.sqrt(tok * seqs)
    vm = pl.BlockSpec(memory_space=pltpu.VMEM)
    hbm = pl.BlockSpec(memory_space=pl.ANY)
    dma = pltpu.SemaphoreType.DMA
    blk = (tok, hd)
    scratch = [
        pltpu.VMEM((2, (nblk + 1) * tok, hd), BF16),
        pltpu.VMEM((heads * tok, hd), BF16),
        pltpu.VMEM((heads * tok, hd), BF16),
        pltpu.VMEM((span, heads * tok), F32),
        pltpu.VMEM((span, heads * tok), F32),
        pltpu.VMEM((span, heads * tok), BF16),
        pltpu.VMEM((span, heads * tok), BF16),
        pltpu.VMEM((5, 2) + blk, F32),
        pltpu.VMEM((4, 2) + blk, BF16),
        pltpu.VMEM((4, 2) + blk, BF16),
        pltpu.VMEM((2, 2) + blk, BF16),
        pltpu.VMEM((2, 2) + blk, BF16),
        pltpu.VMEM((2, 2) + blk, BF16),
        pltpu.VMEM((2, 2) + blk, BF16),
        pltpu.VMEM(blk, BF16),
        pltpu.VMEM(blk, BF16),
        pltpu.VMEM(blk, BF16),
        pltpu.VMEM(blk, BF16),
        pltpu.VMEM(inputs_normed.shape, BF16),
        pltpu.VMEM(kv_weight.shape, BF16),
        pltpu.VMEM((width, tok), BF16),
        pltpu.VMEM((2, group, hd), BF16),
        pltpu.VMEM((2, group, hd), F32),
        pltpu.VMEM((2, group, hd), BF16),
        pltpu.VMEM((planes, rows_out, hd), BF16),
        pltpu.VMEM((planes, rows_out, hd), BF16),
        pltpu.VMEM((planes, rows_out, hd), BF16),
        pltpu.VMEM((planes, rows_out, hd), BF16),
        dma((2,)), dma((2,)),
        dma((2, 2)), dma((2, 2)), dma((2, 2)), dma((2, 2)), dma((5, 2)), dma((5, 2)),
        dma((4, 2)), dma((4, 2)), dma((2, 2)), dma((2, 2)), dma((2, 2)), dma((2, 2)),
        dma((2,)), dma((2,)),
        dma((2,)), dma((2,)), dma((planes,)), dma((planes,)), dma((planes,)), dma((planes,)),
    ]
    query_grad, input_grad, weight = pl.pallas_call(
        functools.partial(kernel, planes, rows_out, heads, norm),
        out_shape=(
            jax.ShapeDtypeStruct(query.shape, BF16),
            jax.ShapeDtypeStruct((tok, kv_weight.shape[1]), BF16),
            jax.ShapeDtypeStruct((rows_out, hd), F32),
        ),
        in_specs=[vm, vm, vm, vm, hbm, hbm],
        out_specs=(vm, vm, vm),
        scratch_shapes=scratch,
        compiler_params=pltpu.CompilerParams(
            collective_id=0, has_side_effects=True, vmem_limit_bytes=60 * 1024 * 1024),
    )(query, key_value, out_grad, lo, inputs_normed, kv_weight)
    return (query_grad, input_grad, weight[None])


def solution(mesh):
    return jax.shard_map(
        local,
        mesh=mesh,
        in_specs=(
            P("seq", "head"),
            P("seq", None),
            P("seq", "head"),
            P("seq", None),
            P(None, "head", None),
            P(),
        ),
        out_specs=(P("seq", "head"), P("seq", "head"), P("head", "seq", None)),
        check_vma=False,
    )
```

```python
import functools
import math

import jax
import jax.numpy as jnp
from jax import lax
from jax.experimental import pallas as pl
from jax.experimental.pallas import tpu as pltpu
from jax.sharding import PartitionSpec as P

WIN = 2048
MESH = pl.DeviceIdType.MESH
F32 = jnp.float32
BF16 = jnp.bfloat16
NT = (((1,), (1,)), ((), ()))
TN = (((0,), (0,)), ((), ()))


def dot(a, b, dims=(((1,), (0,)), ((), ()))):
    return lax.dot_general(a, b, dims, preferred_element_type=F32)


def kernel(planes, rows_out, heads, norm, q_ref, kv_ref, do_ref, seg_ref, x_hbm, w_hbm,
           dq_ref, ig_ref, wg_ref,
           win, qf, dof, top, sc, dp, pb, ds, acc, gs, rc, ys, yr, zs, zr, xs, xr, mh, oh,
           xv, wv, xt, wb, wa, cr, yw, ywr, zw, zwr,
           loc_sem, own_sem, zsend, zrecv, ysend, yrecv, csend, crecv,
           gsend, grecv, bysend, byrecv, bzsend, bzrecv, bxsend, bxrecv,
           wcsend, wcrecv, wysend, wyrecv, wzsend, wzrecv):
    tok = q_ref.shape[0]
    hd = kv_ref.shape[1] // 2
    nblk = WIN // tok + 1
    s_idx = lax.axis_index("seq")
    h_idx = lax.axis_index("head")
    k = s_idx % 2
    y = (s_idx // 2) % 2
    p = s_idx // 4
    core_dev = ((p * 2 + y) * 2 + 1 - k, h_idx)
    y_dev = ((p * 2 + 1 - y) * 2 + k, h_idx)
    x_dev = (s_idx, 1 - h_idx)

    def plane_dev(step):
        return ((((p + step) % planes) * 2 + y) * 2 + k, h_idx)

    next_dev = plane_dev(1)
    prev_dev = plane_dev(planes - 1)

    load_x = pltpu.make_async_copy(x_hbm, xv, loc_sem.at[0])
    load_w = pltpu.make_async_copy(w_hbm, wv, loc_sem.at[1])
    load_x.start()
    load_w.start()

    barrier = pltpu.get_barrier_semaphore()
    for dev in [core_dev, y_dev, x_dev] + [plane_dev(t) for t in range(1, planes)]:
        pl.semaphore_signal(barrier, inc=1, device_id=dev, device_id_type=MESH)
    pl.semaphore_wait(barrier, planes + 2)

    def remote(src, dst, ssem, rsem, dev):
        return pltpu.make_async_remote_copy(
            src_ref=src, dst_ref=dst, send_sem=ssem, recv_sem=rsem,
            device_id=dev, device_id_type=MESH)

    def slot(half, j, core):
        return win.at[half, pl.ds(((4 - j) * 2 + core) * tok, tok)]

    def kv_half(half):
        return kv_ref.at[:, pl.ds(half * hd, hd)]

    def z_own(half):
        return remote(kv_half(half), slot(half, 2, k), zsend.at[0, half], zrecv.at[0, half], next_dev)

    def z_relay(half):
        return remote(slot(half, 2, k), slot(half, 4, k), zsend.at[1, half], zrecv.at[1, half], next_dev)

    def y_first(half, src):
        return remote(src, slot(half, 1, k), ysend.at[0, half], yrecv.at[0, half], y_dev)

    def y_second(half, j):
        return remote(slot(half, j, k), slot(half, 3, k), ysend.at[1, half], yrecv.at[1, half], y_dev)

    def to_core(half, j, src):
        return remote(src, slot(half, j, k), csend.at[j, half], crecv.at[j, half], core_dev)

    def own_fill(half):
        return pltpu.make_async_copy(kv_half(half), slot(half, 0, k), own_sem.at[half])

    def sends_core(j):
        return k == 0 if j == 0 else (k == 1 if j == 4 else None)

    def start_core(half, j, src):
        cond = sends_core(j)
        if cond is None:
            to_core(half, j, src).start()
        else:
            pl.when(cond)(lambda: to_core(half, j, src).start())

    for half in range(2):
        z_own(half).start()
        pl.when(y == 0)(lambda half=half: y_first(half, kv_half(half)).start())
        own_fill(half).start()
        start_core(half, 0, kv_half(half))

    for h in range(heads):
        qf[h * tok:(h + 1) * tok, :] = q_ref[:, h * hd:(h + 1) * hd]
        dof[h * tok:(h + 1) * tok, :] = do_ref[:, h * hd:(h + 1) * hd]

    seg_q = seg_ref[s_idx].astype(F32)
    earlier = jnp.zeros((1, tok), F32)
    for d in range(nblk):
        blk = s_idx - (nblk - 1) + d
        seg_k = seg_ref[jnp.maximum(blk, 0)].astype(F32)
        down = jnp.broadcast_to(seg_k, (tok, tok)).T
        less = jnp.sum((down < seg_q).astype(F32), axis=0, keepdims=True)
        earlier = earlier + jnp.where(blk >= 0, less, float(tok))
    col = lax.broadcasted_iota(jnp.int32, (1, tok), 1)
    lo = jnp.maximum(earlier.astype(jnp.int32), col + 1)
    hi = col + WIN
    inv_root = 1.0 / math.sqrt(hd)
    top[...] = jnp.full(top.shape, -jnp.inf, F32)

    def block_rows(d):
        return pl.ds(pl.multiple_of((k + d) * tok, tok), tok)

    def own_rows(d):
        return pl.ds(pl.multiple_of(d * tok, tok), tok)

    def block_scores(d):
        keys = win[0, block_rows(d), :]
        vals = win[1, block_rows(d), :]
        r = lax.broadcasted_iota(jnp.int32, (tok, tok), 0) + d * tok
        ok = (r >= lo) & (r <= hi)
        for h in range(heads):
            cols = slice(h * tok, (h + 1) * tok)
            s = jnp.where(ok, dot(keys, qf[cols, :], NT) * inv_root, -jnp.inf)
            sc[own_rows(d), cols] = s
            top[:, cols] = jnp.maximum(top[:, cols], jnp.max(s, axis=0, keepdims=True))
            dp[own_rows(d), cols] = dot(vals, dof[cols, :], NT)

    def own_scores(j):
        block_scores(8 - 2 * j)

    def partner_scores(j):
        def run():
            for half in range(2):
                to_core(half, j, slot(half, j, k)).wait_recv()
            block_scores(9 - 2 * j - 2 * k)

        if j == 0:
            pl.when(k == 1)(run)
        elif j == 4:
            pl.when(k == 0)(run)
        else:
            run()

    per = max(1, 256 // rows_out)
    wide = per * rows_out
    pieces = xv.shape[1] // wide

    def transpose_inputs(first, last):
        for i in range(first, last):
            piece = xv[:, i * wide:(i + 1) * wide].T
            for u in range(per):
                dest = i * per + u
                place = ((dest % 2) * 2 + (dest // 2) % 2) * planes + dest // 4
                xt[place * rows_out:(place + 1) * rows_out, :] = piece[u * rows_out:(u + 1) * rows_out]

    for half in range(2):
        own_fill(half).wait()
    own_scores(0)
    partner_scores(0)
    for half in range(2):
        z_own(half).wait_recv()
        z_relay(half).start()

        @pl.when(y == 0)
        def _(half=half):
            y_second(half, 2).start()

        @pl.when(y == 1)
        def _(half=half):
            y_first(half, slot(half, 2, k)).start()

        start_core(half, 2, slot(half, 2, k))
    own_scores(2)
    load_x.wait()
    transpose_inputs(0, pieces // 2)
    for half in range(2):
        y_first(half, kv_half(half)).wait_recv()
        start_core(half, 1, slot(half, 1, k))
    partner_scores(2)
    own_scores(1)
    for half in range(2):
        z_relay(half).wait_recv()
        pl.when(y == 1)(lambda half=half: y_second(half, 4).start())
        start_core(half, 4, slot(half, 4, k))
    own_scores(4)
    partner_scores(1)
    transpose_inputs(pieces // 2, pieces)
    partner_scores(4)
    for half in range(2):
        y_second(half, 2).wait_recv()
        start_core(half, 3, slot(half, 3, k))
    own_scores(3)
    partner_scores(3)

    tops = [top[:, h * tok:(h + 1) * tok] for h in range(heads)]

    def pass_exp(d, sums):
        out = []
        for h in range(heads):
            cols = slice(h * tok, (h + 1) * tok)
            e = jnp.exp(sc[own_rows(d), cols] - tops[h])
            sc[own_rows(d), cols] = e
            out.append((sums[h][0] + jnp.sum(e, axis=0, keepdims=True),
                        sums[h][1] + jnp.sum(e * dp[own_rows(d), cols], axis=0, keepdims=True)))
        return tuple(out)

    zero = jnp.zeros((1, tok), F32)
    sums = lax.fori_loop(0, nblk, pass_exp, tuple((zero, zero) for _ in range(heads)))
    invs = [1.0 / total for total, _ in sums]
    deltas = [part * inv for (_, part), inv in zip(sums, invs)]

    def pass_grad(d):
        for h in range(heads):
            cols = slice(h * tok, (h + 1) * tok)
            prob = sc[own_rows(d), cols] * invs[h]
            pb[own_rows(d), cols] = prob.astype(BF16)
            ds[own_rows(d), cols] = (prob * (dp[own_rows(d), cols] - deltas[h])).astype(BF16)

    def grad_of(d, half):
        if half == 0:
            return dot(ds[own_rows(d), :], qf[...]) * inv_root
        return dot(pb[own_rows(d), :], dof[...])

    def g_copy(m, half):
        return remote(gs.at[m, half], rc.at[m, half], gsend.at[m, half], grecv.at[m, half], core_dev)

    def send_grad(m):
        pass_grad(2 * m + 1)
        for half in range(2):
            gs[m, half] = grad_of(2 * m + 1, half).astype(BF16)
            g_copy(m, half).start()

    def own_grad(j):
        pass_grad(8 - 2 * j)
        for half in range(2):
            acc[j, half] = grad_of(8 - 2 * j, half)

    def x_copy(j):
        return remote(xs.at[j], xr.at[j], bxsend.at[j], bxrecv.at[j], x_dev)

    def y_copy(i):
        return remote(ys.at[i], yr.at[i], bysend.at[i], byrecv.at[i], y_dev)

    def z_copy(i):
        return remote(zs.at[i], zr.at[i], bzsend.at[i], bzrecv.at[i], prev_dev)

    def to_x(j):
        def add():
            m = 3 + k - j if 0 < j < 4 else (0 if j == 4 else 3)
            for half in range(2):
                g_copy(m, half).wait_recv()
                acc[j, half] = acc[j, half] + rc[m, half].astype(F32)

        if j == 0:
            pl.when(k == 0)(add)
        elif j == 4:
            pl.when(k == 1)(add)
        else:
            add()
        xs[j] = acc[j, 1 - h_idx].astype(BF16)
        x_copy(j).start()

    def from_x(j):
        x_copy(j).wait_recv()
        acc[j, h_idx] = acc[j, h_idx] + xr[j].astype(F32)

    def to_y(i, j):
        from_x(j)
        ys[i] = acc[j, h_idx].astype(BF16)
        y_copy(i).start()

    def from_y(i):
        y_copy(i).wait_recv()
        acc[2 * i + 2 * y, h_idx] = acc[2 * i + 2 * y, h_idx] + yr[i].astype(F32)

    send_grad(1 - k)
    own_grad(3)
    send_grad(3 - k)
    to_x(3)
    own_grad(1)
    send_grad(3 * k)
    to_x(1)
    own_grad(4)
    send_grad(2 - k)
    to_x(4)
    own_grad(2)
    to_x(2)
    own_grad(0)
    to_x(0)
    to_y(1, 3)
    to_y(0, 1)
    keys_all = win[0, pl.ds(pl.multiple_of(k * tok, tok), nblk * tok), :]

    def query_part(h):
        cols = slice(h * tok, (h + 1) * tok)
        dq_ref[:, h * hd:(h + 1) * hd] = (dot(ds[:, cols], keys_all, TN) * inv_root).astype(BF16)

    for h in range(heads // 2):
        query_part(h)
    from_x(4)
    from_x(2)
    from_y(1)
    zs[1] = acc[4, h_idx].astype(BF16)
    z_copy(1).start()
    for h in range(heads // 2, heads):
        query_part(h)
    from_x(0)
    from_y(0)
    z_copy(1).wait_recv()
    zs[0] = (acc[2, h_idx] + zr[1].astype(F32)).astype(BF16)
    z_copy(0).start()
    z_copy(0).wait_recv()
    mh[...] = (acc[0, h_idx] + zr[0].astype(F32)).astype(BF16)
    x_back = remote(mh, oh, bxsend.at[5], bxrecv.at[5], x_dev)

    group = planes * rows_out
    half_rows = 2 * group

    def w_core(i):
        return remote(wb.at[i], cr.at[i], wcsend.at[i], wcrecv.at[i], core_dev)

    def xt_rows(core, yy):
        return xt[pl.ds(pl.multiple_of((core * 2 + yy) * group, group), group), :]

    def w_y(t):
        return remote(yw.at[t], ywr.at[t], wysend.at[t], wyrecv.at[t], y_dev)

    def w_z(t):
        return remote(zw.at[t], zwr.at[t], wzsend.at[t], wzrecv.at[t], plane_dev(t))

    for i in range(2):
        yy = 1 - y if i == 0 else y
        wb[i] = dot(xt_rows(1 - k, yy), mh[...]).astype(BF16)
        w_core(i).start()
    x_back.start()
    for i in range(2):
        yy = 1 - y if i == 0 else y
        wa[i] = dot(xt_rows(k, yy), mh[...])

    order = list(range(1, planes)) + [0]

    def plane_rows(t):
        return pl.ds(pl.multiple_of(((p + t) % planes) * rows_out, rows_out), rows_out)

    w_core(0).wait_recv()
    for t in order:
        yw[t] = (wa[0, plane_rows(t), :] + cr[0, plane_rows(t), :].astype(F32)).astype(BF16)
        w_y(t).start()
    w_core(1).wait_recv()
    wa[1] = wa[1] + cr[1].astype(F32)

    load_w.wait()
    x_back.wait_recv()
    first = jnp.where(h_idx == 0, mh[...].astype(F32), oh[...].astype(F32)).astype(BF16)
    second = jnp.where(h_idx == 0, oh[...].astype(F32), mh[...].astype(F32)).astype(BF16)
    width = wv.shape[1]
    step = 512
    for i in range(width // step):
        cols = slice(i * step, (i + 1) * step)
        ig_ref[:, cols] = (dot(first, wv[0, cols, :], NT) + dot(second, wv[1, cols, :], NT)).astype(BF16)

    for t in order[:-1]:
        w_y(t).wait_recv()
        zw[t] = (wa[1, plane_rows(t), :] + ywr[t].astype(F32)).astype(BF16)
        w_z(t).start()
    w_y(0).wait_recv()
    total = wa[1, plane_rows(0), :] + ywr[0].astype(F32)
    for t in order[:-1]:
        w_z(t).wait_recv()
        total = total + zwr[t].astype(F32)
    wg_ref[...] = total * norm

    for half in range(2):
        z_own(half).wait_send()
        z_relay(half).wait_send()
        y_first(half, kv_half(half)).wait_send()
        y_second(half, 2).wait_send()
        for j in range(1, 4):
            to_core(half, j, slot(half, j, k)).wait_send()
        pl.when(k == 0)(lambda half=half: to_core(half, 0, slot(half, 0, k)).wait_send())
        pl.when(k == 1)(lambda half=half: to_core(half, 4, slot(half, 4, k)).wait_send())
        for m in range(4):
            g_copy(m, half).wait_send()
    for i in range(2):
        y_copy(i).wait_send()
        z_copy(i).wait_send()
    for j in range(5):
        x_copy(j).wait_send()
    x_back.wait_send()
    for i in range(2):
        w_core(i).wait_send()
    for t in order:
        w_y(t).wait_send()
    for t in order[:-1]:
        w_z(t).wait_send()


def put_out(a_ref, b_ref, c_ref, a_out, b_out, c_out, sem):
    copies = [pltpu.make_async_copy(a_ref, a_out, sem.at[0]),
              pltpu.make_async_copy(b_ref, b_out, sem.at[1]),
              pltpu.make_async_copy(c_ref, c_out, sem.at[2])]
    for copy in copies:
        copy.start()
    for copy in copies:
        copy.wait()


def local(query, key_value, out_grad, inputs_normed, kv_weight, segment_ids):
    tok = query.shape[0]
    hd = key_value.shape[1] // 2
    heads = query.shape[1] // hd
    seqs = lax.axis_size("seq")
    planes = seqs // 4
    width = inputs_normed.shape[1]
    rows_out = width // seqs
    span = WIN + tok
    nblk = span // tok
    group = planes * rows_out
    seg = segment_ids.reshape(seqs, 1, tok)
    norm = 1.0 / math.sqrt(tok * seqs)
    vm = pl.BlockSpec(memory_space=pltpu.VMEM)
    hbm = pl.BlockSpec(memory_space=pl.ANY)
    dma = pltpu.SemaphoreType.DMA
    blk = (tok, hd)
    scratch = [
        pltpu.VMEM((2, (nblk + 1) * tok, hd), BF16),
        pltpu.VMEM((heads * tok, hd), BF16),
        pltpu.VMEM((heads * tok, hd), BF16),
        pltpu.VMEM((1, heads * tok), F32),
        pltpu.VMEM((span, heads * tok), F32),
        pltpu.VMEM((span, heads * tok), F32),
        pltpu.VMEM((span, heads * tok), BF16),
        pltpu.VMEM((span, heads * tok), BF16),
        pltpu.VMEM((5, 2) + blk, F32),
        pltpu.VMEM((4, 2) + blk, BF16),
        pltpu.VMEM((4, 2) + blk, BF16),
        pltpu.VMEM((2,) + blk, BF16),
        pltpu.VMEM((2,) + blk, BF16),
        pltpu.VMEM((2,) + blk, BF16),
        pltpu.VMEM((2,) + blk, BF16),
        pltpu.VMEM((5,) + blk, BF16),
        pltpu.VMEM((5,) + blk, BF16),
        pltpu.VMEM(blk, BF16),
        pltpu.VMEM(blk, BF16),
        pltpu.VMEM(inputs_normed.shape, BF16),
        pltpu.VMEM(kv_weight.shape, BF16),
        pltpu.VMEM((width, tok), BF16),
        pltpu.VMEM((2, group, hd), BF16),
        pltpu.VMEM((2, group, hd), F32),
        pltpu.VMEM((2, group, hd), BF16),
        pltpu.VMEM((planes, rows_out, hd), BF16),
        pltpu.VMEM((planes, rows_out, hd), BF16),
        pltpu.VMEM((planes, rows_out, hd), BF16),
        pltpu.VMEM((planes, rows_out, hd), BF16),
        dma((2,)), dma((2,)),
        dma((2, 2)), dma((2, 2)), dma((2, 2)), dma((2, 2)), dma((5, 2)), dma((5, 2)),
        dma((4, 2)), dma((4, 2)), dma((2,)), dma((2,)), dma((2,)), dma((2,)),
        dma((6,)), dma((6,)),
        dma((2,)), dma((2,)), dma((planes,)), dma((planes,)), dma((planes,)), dma((planes,)),
    ]
    query_grad, input_grad, weight = pl.pallas_call(
        functools.partial(kernel, planes, rows_out, heads, norm),
        out_shape=(
            jax.ShapeDtypeStruct(query.shape, BF16),
            jax.ShapeDtypeStruct((tok, kv_weight.shape[1]), BF16),
            jax.ShapeDtypeStruct((rows_out, hd), F32),
        ),
        in_specs=[vm, vm, vm, vm, hbm, hbm],
        out_specs=(vm, vm, vm),
        scratch_shapes=scratch,
        compiler_params=pltpu.CompilerParams(
            collective_id=0, has_side_effects=True, vmem_limit_bytes=60 * 1024 * 1024),
    )(query, key_value, out_grad, seg, inputs_normed, kv_weight)
    results = (query_grad, input_grad, weight)
    query_grad, input_grad, weight = pl.pallas_call(
        put_out,
        out_shape=tuple(jax.ShapeDtypeStruct(r.shape, r.dtype) for r in results),
        in_specs=[vm, vm, vm],
        out_specs=(hbm, hbm, hbm),
        scratch_shapes=[dma((3,))],
    )(*results)
    return (query_grad, input_grad, weight[None])


def solution(mesh):
    return jax.shard_map(
        local,
        mesh=mesh,
        in_specs=(
            P("seq", "head"),
            P("seq", None),
            P("seq", "head"),
            P("seq", None),
            P(None, "head", None),
            P(),
        ),
        out_specs=(P("seq", "head"), P("seq", "head"), P("head", "seq", None)),
        check_vma=False,
    )
```

```python
import functools
import math

import jax
import jax.numpy as jnp
from jax import lax
from jax.experimental import pallas as pl
from jax.experimental.pallas import tpu as pltpu
from jax.sharding import PartitionSpec as P

WIN = 2048
MESH = pl.DeviceIdType.MESH
F32 = jnp.float32
BF16 = jnp.bfloat16
NT = (((1,), (1,)), ((), ()))
TN = (((0,), (0,)), ((), ()))


def dot(a, b, dims=(((1,), (0,)), ((), ()))):
    return lax.dot_general(a, b, dims, preferred_element_type=F32)


def kernel(planes, rows_out, heads, norm, q_ref, kv_ref, do_ref, seg_ref, x_hbm, w_hbm,
           dq_ref, ig_ref, wg_ref,
           win, qf, dof, top, sc, dp, pb, ds, acc, gs, rc, ys, yr, zs, zr, xs, xr, mh, oh,
           xv, wv, xt, wb, wa, cr, yw, ywr, zw, zwr, dqv, igv,
           loc_sem, in_sem, own_sem, zsend, zrecv, ysend, yrecv, csend, crecv,
           gsend, grecv, bysend, byrecv, bzsend, bzrecv, bxsend, bxrecv,
           wcsend, wcrecv, wysend, wyrecv, wzsend, wzrecv):
    tok = kv_ref.shape[0]
    hd = kv_ref.shape[1] // 2
    nblk = WIN // tok + 1
    s_idx = lax.axis_index("seq")
    h_idx = lax.axis_index("head")
    k = s_idx % 2
    y = (s_idx // 2) % 2
    p = s_idx // 4
    core_dev = ((p * 2 + y) * 2 + 1 - k, h_idx)
    y_dev = ((p * 2 + 1 - y) * 2 + k, h_idx)
    x_dev = (s_idx, 1 - h_idx)

    def plane_dev(step):
        return ((((p + step) % planes) * 2 + y) * 2 + k, h_idx)

    next_dev = plane_dev(1)
    prev_dev = plane_dev(planes - 1)

    load_x = pltpu.make_async_copy(x_hbm, xv, loc_sem.at[0])
    load_w = pltpu.make_async_copy(w_hbm, wv, loc_sem.at[1])
    loads = []
    for h in range(heads):
        for i, (src, dst) in enumerate(((q_ref, qf), (do_ref, dof))):
            loads.append(pltpu.make_async_copy(
                src.at[:, pl.ds(h * hd, hd)], dst.at[pl.ds(h * tok, tok)], in_sem.at[i, h]))
    for load in loads:
        load.start()
    load_x.start()
    load_w.start()
    put_q = pltpu.make_async_copy(dqv, dq_ref, loc_sem.at[2])
    put_i = pltpu.make_async_copy(igv, ig_ref, loc_sem.at[3])

    barrier = pltpu.get_barrier_semaphore()
    for dev in [core_dev, y_dev, x_dev] + [plane_dev(t) for t in range(1, planes)]:
        pl.semaphore_signal(barrier, inc=1, device_id=dev, device_id_type=MESH)
    pl.semaphore_wait(barrier, planes + 2)

    def remote(src, dst, ssem, rsem, dev):
        return pltpu.make_async_remote_copy(
            src_ref=src, dst_ref=dst, send_sem=ssem, recv_sem=rsem,
            device_id=dev, device_id_type=MESH)

    def slot(half, j, core):
        return win.at[half, pl.ds(((4 - j) * 2 + core) * tok, tok)]

    def kv_half(half):
        return kv_ref.at[:, pl.ds(half * hd, hd)]

    def z_own(half):
        return remote(kv_half(half), slot(half, 2, k), zsend.at[0, half], zrecv.at[0, half], next_dev)

    def z_relay(half):
        return remote(slot(half, 2, k), slot(half, 4, k), zsend.at[1, half], zrecv.at[1, half], next_dev)

    def y_first(half, src):
        return remote(src, slot(half, 1, k), ysend.at[0, half], yrecv.at[0, half], y_dev)

    def y_second(half, j):
        return remote(slot(half, j, k), slot(half, 3, k), ysend.at[1, half], yrecv.at[1, half], y_dev)

    def to_core(half, j, src):
        return remote(src, slot(half, j, k), csend.at[j, half], crecv.at[j, half], core_dev)

    def own_fill(half):
        return pltpu.make_async_copy(kv_half(half), slot(half, 0, k), own_sem.at[half])

    def sends_core(j):
        return k == 0 if j == 0 else (k == 1 if j == 4 else None)

    def start_core(half, j, src):
        cond = sends_core(j)
        if cond is None:
            to_core(half, j, src).start()
        else:
            pl.when(cond)(lambda: to_core(half, j, src).start())

    for half in range(2):
        z_own(half).start()
        pl.when(y == 0)(lambda half=half: y_first(half, kv_half(half)).start())
        own_fill(half).start()
        start_core(half, 0, kv_half(half))

    seg_q = seg_ref[s_idx].astype(F32)
    earlier = jnp.zeros((1, tok), F32)
    for d in range(nblk):
        blk = s_idx - (nblk - 1) + d
        seg_k = seg_ref[jnp.maximum(blk, 0)].astype(F32)
        down = jnp.broadcast_to(seg_k, (tok, tok)).T
        less = jnp.sum((down < seg_q).astype(F32), axis=0, keepdims=True)
        earlier = earlier + jnp.where(blk >= 0, less, float(tok))
    col = lax.broadcasted_iota(jnp.int32, (1, tok), 1)
    lo = jnp.maximum(earlier.astype(jnp.int32), col + 1)
    hi = col + WIN
    inv_root = 1.0 / math.sqrt(hd)
    top[...] = jnp.full(top.shape, -jnp.inf, F32)

    def block_rows(d):
        return pl.ds(pl.multiple_of((k + d) * tok, tok), tok)

    def own_rows(d):
        return pl.ds(pl.multiple_of(d * tok, tok), tok)

    def block_scores(d):
        keys = win[0, block_rows(d), :]
        vals = win[1, block_rows(d), :]
        r = lax.broadcasted_iota(jnp.int32, (tok, tok), 0) + d * tok
        ok = (r >= lo) & (r <= hi)
        for h in range(heads):
            cols = slice(h * tok, (h + 1) * tok)
            s = jnp.where(ok, dot(keys, qf[cols, :], NT) * inv_root, -jnp.inf)
            sc[own_rows(d), cols] = s
            top[:, cols] = jnp.maximum(top[:, cols], jnp.max(s, axis=0, keepdims=True))
            dp[own_rows(d), cols] = dot(vals, dof[cols, :], NT)

    def own_scores(j):
        block_scores(8 - 2 * j)

    def partner_scores(j):
        def run():
            for half in range(2):
                to_core(half, j, slot(half, j, k)).wait_recv()
            block_scores(9 - 2 * j - 2 * k)

        if j == 0:
            pl.when(k == 1)(run)
        elif j == 4:
            pl.when(k == 0)(run)
        else:
            run()

    per = max(1, 256 // rows_out)
    wide = per * rows_out
    pieces = xv.shape[1] // wide

    def transpose_inputs(first, last):
        for i in range(first, last):
            piece = xv[:, i * wide:(i + 1) * wide].T
            for u in range(per):
                dest = i * per + u
                place = ((dest % 2) * 2 + (dest // 2) % 2) * planes + dest // 4
                xt[place * rows_out:(place + 1) * rows_out, :] = piece[u * rows_out:(u + 1) * rows_out]

    for load in loads:
        load.wait()
    for half in range(2):
        own_fill(half).wait()
    own_scores(0)
    partner_scores(0)
    for half in range(2):
        z_own(half).wait_recv()
        z_relay(half).start()

        @pl.when(y == 0)
        def _(half=half):
            y_second(half, 2).start()

        @pl.when(y == 1)
        def _(half=half):
            y_first(half, slot(half, 2, k)).start()

        start_core(half, 2, slot(half, 2, k))
    own_scores(2)
    load_x.wait()
    transpose_inputs(0, pieces // 2)
    for half in range(2):
        y_first(half, kv_half(half)).wait_recv()
        start_core(half, 1, slot(half, 1, k))
    partner_scores(2)
    own_scores(1)
    for half in range(2):
        z_relay(half).wait_recv()
        pl.when(y == 1)(lambda half=half: y_second(half, 4).start())
        start_core(half, 4, slot(half, 4, k))
    own_scores(4)
    partner_scores(1)
    transpose_inputs(pieces // 2, pieces)
    partner_scores(4)
    for half in range(2):
        y_second(half, 2).wait_recv()
        start_core(half, 3, slot(half, 3, k))
    own_scores(3)
    partner_scores(3)

    tops = [top[:, h * tok:(h + 1) * tok] for h in range(heads)]

    def pass_exp(d, sums):
        out = []
        for h in range(heads):
            cols = slice(h * tok, (h + 1) * tok)
            e = jnp.exp(sc[own_rows(d), cols] - tops[h])
            sc[own_rows(d), cols] = e
            out.append((sums[h][0] + jnp.sum(e, axis=0, keepdims=True),
                        sums[h][1] + jnp.sum(e * dp[own_rows(d), cols], axis=0, keepdims=True)))
        return tuple(out)

    zero = jnp.zeros((1, tok), F32)
    sums = lax.fori_loop(0, nblk, pass_exp, tuple((zero, zero) for _ in range(heads)))
    invs = [1.0 / total for total, _ in sums]
    deltas = [part * inv for (_, part), inv in zip(sums, invs)]

    def pass_grad(d):
        for h in range(heads):
            cols = slice(h * tok, (h + 1) * tok)
            prob = sc[own_rows(d), cols] * invs[h]
            pb[own_rows(d), cols] = prob.astype(BF16)
            ds[own_rows(d), cols] = (prob * (dp[own_rows(d), cols] - deltas[h])).astype(BF16)

    def grad_of(d, half):
        if half == 0:
            return dot(ds[own_rows(d), :], qf[...]) * inv_root
        return dot(pb[own_rows(d), :], dof[...])

    def g_copy(m, half):
        return remote(gs.at[m, half], rc.at[m, half], gsend.at[m, half], grecv.at[m, half], core_dev)

    def send_grad(m):
        pass_grad(2 * m + 1)
        for half in range(2):
            gs[m, half] = grad_of(2 * m + 1, half).astype(BF16)
            g_copy(m, half).start()

    def own_grad(j):
        pass_grad(8 - 2 * j)
        for half in range(2):
            acc[j, half] = grad_of(8 - 2 * j, half)

    def x_copy(j):
        return remote(xs.at[j], xr.at[j], bxsend.at[j], bxrecv.at[j], x_dev)

    def y_copy(i):
        return remote(ys.at[i], yr.at[i], bysend.at[i], byrecv.at[i], y_dev)

    def z_copy(i):
        return remote(zs.at[i], zr.at[i], bzsend.at[i], bzrecv.at[i], prev_dev)

    def to_x(j):
        def add():
            m = 3 + k - j if 0 < j < 4 else (0 if j == 4 else 3)
            for half in range(2):
                g_copy(m, half).wait_recv()
                acc[j, half] = acc[j, half] + rc[m, half].astype(F32)

        if j == 0:
            pl.when(k == 0)(add)
        elif j == 4:
            pl.when(k == 1)(add)
        else:
            add()
        xs[j] = acc[j, 1 - h_idx].astype(BF16)
        x_copy(j).start()

    def from_x(j):
        x_copy(j).wait_recv()
        acc[j, h_idx] = acc[j, h_idx] + xr[j].astype(F32)

    def to_y(i, j):
        from_x(j)
        ys[i] = acc[j, h_idx].astype(BF16)
        y_copy(i).start()

    def from_y(i):
        y_copy(i).wait_recv()
        acc[2 * i + 2 * y, h_idx] = acc[2 * i + 2 * y, h_idx] + yr[i].astype(F32)

    send_grad(1 - k)
    own_grad(3)
    send_grad(3 - k)
    to_x(3)
    own_grad(1)
    send_grad(3 * k)
    to_x(1)
    own_grad(4)
    send_grad(2 - k)
    to_x(4)
    own_grad(2)
    to_x(2)
    own_grad(0)
    to_x(0)
    to_y(1, 3)
    to_y(0, 1)
    keys_all = win[0, pl.ds(pl.multiple_of(k * tok, tok), nblk * tok), :]

    def query_part(h):
        cols = slice(h * tok, (h + 1) * tok)
        dqv[:, h * hd:(h + 1) * hd] = (dot(ds[:, cols], keys_all, TN) * inv_root).astype(BF16)

    for h in range(heads // 2):
        query_part(h)
    from_x(4)
    from_x(2)
    from_y(1)
    zs[1] = acc[4, h_idx].astype(BF16)
    z_copy(1).start()
    for h in range(heads // 2, heads):
        query_part(h)
    put_q.start()
    from_x(0)
    from_y(0)
    z_copy(1).wait_recv()
    zs[0] = (acc[2, h_idx] + zr[1].astype(F32)).astype(BF16)
    z_copy(0).start()
    z_copy(0).wait_recv()
    mh[...] = (acc[0, h_idx] + zr[0].astype(F32)).astype(BF16)
    x_back = remote(mh, oh, bxsend.at[5], bxrecv.at[5], x_dev)

    group = planes * rows_out
    half_rows = 2 * group

    def w_core(i):
        return remote(wb.at[i], cr.at[i], wcsend.at[i], wcrecv.at[i], core_dev)

    def xt_rows(core, yy):
        return xt[pl.ds(pl.multiple_of((core * 2 + yy) * group, group), group), :]

    def w_y(t):
        return remote(yw.at[t], ywr.at[t], wysend.at[t], wyrecv.at[t], y_dev)

    def w_z(t):
        return remote(zw.at[t], zwr.at[t], wzsend.at[t], wzrecv.at[t], plane_dev(t))

    for i in range(2):
        yy = 1 - y if i == 0 else y
        wb[i] = dot(xt_rows(1 - k, yy), mh[...]).astype(BF16)
        w_core(i).start()
    x_back.start()
    for i in range(2):
        yy = 1 - y if i == 0 else y
        wa[i] = dot(xt_rows(k, yy), mh[...])

    order = list(range(1, planes)) + [0]

    def plane_rows(t):
        return pl.ds(pl.multiple_of(((p + t) % planes) * rows_out, rows_out), rows_out)

    w_core(0).wait_recv()
    for t in order:
        yw[t] = (wa[0, plane_rows(t), :] + cr[0, plane_rows(t), :].astype(F32)).astype(BF16)
        w_y(t).start()
    w_core(1).wait_recv()
    wa[1] = wa[1] + cr[1].astype(F32)

    load_w.wait()
    x_back.wait_recv()
    first = jnp.where(h_idx == 0, mh[...].astype(F32), oh[...].astype(F32)).astype(BF16)
    second = jnp.where(h_idx == 0, oh[...].astype(F32), mh[...].astype(F32)).astype(BF16)
    width = wv.shape[1]
    step = 512
    for i in range(width // step):
        cols = slice(i * step, (i + 1) * step)
        igv[:, cols] = (dot(first, wv[0, cols, :], NT) + dot(second, wv[1, cols, :], NT)).astype(BF16)

    put_i.start()
    for t in order[:-1]:
        w_y(t).wait_recv()
        zw[t] = (wa[1, plane_rows(t), :] + ywr[t].astype(F32)).astype(BF16)
        w_z(t).start()
    w_y(0).wait_recv()
    total = wa[1, plane_rows(0), :] + ywr[0].astype(F32)
    for t in order[:-1]:
        w_z(t).wait_recv()
        total = total + zwr[t].astype(F32)
    wg_ref[...] = total * norm

    put_q.wait()
    put_i.wait()
    for half in range(2):
        z_own(half).wait_send()
        z_relay(half).wait_send()
        y_first(half, kv_half(half)).wait_send()
        y_second(half, 2).wait_send()
        for j in range(1, 4):
            to_core(half, j, slot(half, j, k)).wait_send()
        pl.when(k == 0)(lambda half=half: to_core(half, 0, slot(half, 0, k)).wait_send())
        pl.when(k == 1)(lambda half=half: to_core(half, 4, slot(half, 4, k)).wait_send())
        for m in range(4):
            g_copy(m, half).wait_send()
    for i in range(2):
        y_copy(i).wait_send()
        z_copy(i).wait_send()
    for j in range(5):
        x_copy(j).wait_send()
    x_back.wait_send()
    for i in range(2):
        w_core(i).wait_send()
    for t in order:
        w_y(t).wait_send()
    for t in order[:-1]:
        w_z(t).wait_send()


def put_out(*refs):
    sources, results, buffers, sems = refs[:3], refs[3:6], refs[6:9], refs[9]
    fills, drains = [], []
    for i in range(3):
        half = sources[i].shape[0] // 2
        for j in range(2):
            part = pl.ds(j * half, half)
            fills.append(pltpu.make_async_copy(
                sources[i].at[part], buffers[i].at[part], sems.at[0, i, j]))
            drains.append(pltpu.make_async_copy(
                buffers[i].at[part], results[i].at[part], sems.at[1, i, j]))
    for fill in fills:
        fill.start()
    for fill, drain in zip(fills, drains):
        fill.wait()
        drain.start()
    for drain in drains:
        drain.wait()


def local(query, key_value, out_grad, inputs_normed, kv_weight, segment_ids):
    tok = query.shape[0]
    hd = key_value.shape[1] // 2
    heads = query.shape[1] // hd
    seqs = lax.axis_size("seq")
    planes = seqs // 4
    width = inputs_normed.shape[1]
    rows_out = width // seqs
    span = WIN + tok
    nblk = span // tok
    group = planes * rows_out
    seg = segment_ids.reshape(seqs, 1, tok)
    norm = 1.0 / math.sqrt(tok * seqs)
    vm = pl.BlockSpec(memory_space=pltpu.VMEM)
    hbm = pl.BlockSpec(memory_space=pl.ANY)
    dma = pltpu.SemaphoreType.DMA
    blk = (tok, hd)
    scratch = [
        pltpu.VMEM((2, (nblk + 1) * tok, hd), BF16),
        pltpu.VMEM((heads * tok, hd), BF16),
        pltpu.VMEM((heads * tok, hd), BF16),
        pltpu.VMEM((1, heads * tok), F32),
        pltpu.VMEM((span, heads * tok), F32),
        pltpu.VMEM((span, heads * tok), F32),
        pltpu.VMEM((span, heads * tok), BF16),
        pltpu.VMEM((span, heads * tok), BF16),
        pltpu.VMEM((5, 2) + blk, F32),
        pltpu.VMEM((4, 2) + blk, BF16),
        pltpu.VMEM((4, 2) + blk, BF16),
        pltpu.VMEM((2,) + blk, BF16),
        pltpu.VMEM((2,) + blk, BF16),
        pltpu.VMEM((2,) + blk, BF16),
        pltpu.VMEM((2,) + blk, BF16),
        pltpu.VMEM((5,) + blk, BF16),
        pltpu.VMEM((5,) + blk, BF16),
        pltpu.VMEM(blk, BF16),
        pltpu.VMEM(blk, BF16),
        pltpu.VMEM(inputs_normed.shape, BF16),
        pltpu.VMEM(kv_weight.shape, BF16),
        pltpu.VMEM((width, tok), BF16),
        pltpu.VMEM((2, group, hd), BF16),
        pltpu.VMEM((2, group, hd), F32),
        pltpu.VMEM((2, group, hd), BF16),
        pltpu.VMEM((planes, rows_out, hd), BF16),
        pltpu.VMEM((planes, rows_out, hd), BF16),
        pltpu.VMEM((planes, rows_out, hd), BF16),
        pltpu.VMEM((planes, rows_out, hd), BF16),
        pltpu.VMEM(query.shape, BF16),
        pltpu.VMEM((tok, kv_weight.shape[1]), BF16),
        dma((4,)), dma((2, heads)), dma((2,)),
        dma((2, 2)), dma((2, 2)), dma((2, 2)), dma((2, 2)), dma((5, 2)), dma((5, 2)),
        dma((4, 2)), dma((4, 2)), dma((2,)), dma((2,)), dma((2,)), dma((2,)),
        dma((6,)), dma((6,)),
        dma((2,)), dma((2,)), dma((planes,)), dma((planes,)), dma((planes,)), dma((planes,)),
    ]
    query_grad, input_grad, weight = pl.pallas_call(
        functools.partial(kernel, planes, rows_out, heads, norm),
        out_shape=(
            jax.ShapeDtypeStruct(query.shape, BF16),
            jax.ShapeDtypeStruct((tok, kv_weight.shape[1]), BF16),
            jax.ShapeDtypeStruct((rows_out, hd), F32),
        ),
        in_specs=[hbm, vm, hbm, vm, hbm, hbm],
        out_specs=(hbm, hbm, vm),
        scratch_shapes=scratch,
        compiler_params=pltpu.CompilerParams(
            collective_id=0, has_side_effects=True, vmem_limit_bytes=60 * 1024 * 1024),
    )(query, key_value, out_grad, seg, inputs_normed, kv_weight)
    results = (query_grad, input_grad, weight)
    query_grad, input_grad, weight = pl.pallas_call(
        put_out,
        out_shape=tuple(jax.ShapeDtypeStruct(r.shape, r.dtype) for r in results),
        in_specs=[hbm, hbm, hbm],
        out_specs=(hbm, hbm, hbm),
        scratch_shapes=[pltpu.VMEM(r.shape, r.dtype) for r in results] + [dma((2, 3, 2))],
    )(*results)
    return (query_grad, input_grad, weight[None])


def solution(mesh):
    return jax.shard_map(
        local,
        mesh=mesh,
        in_specs=(
            P("seq", "head"),
            P("seq", None),
            P("seq", "head"),
            P("seq", None),
            P(None, "head", None),
            P(),
        ),
        out_specs=(P("seq", "head"), P("seq", "head"), P("head", "seq", None)),
        check_vma=False,
    )
```
